32 devices in a mesh: tm: 8 (over z, x), chan: 4 (over y, core).
Axes of the slice: x: 2, y: 2, z: 4, core: 2. Of those that a mesh axis runs over, the one named last changes fastest.
Arguments:
- surveillance: bfloat16 [128, 1024, 256], P(('chan', 'tm')), parts along dimension 0, may hold values from -6 to 6
- ref_samples: bfloat16 [32, 1040, 256], P('tm'), may hold values from -6 to 6
- block_ids: int32 [32], P('tm'), may hold values from 0 to 31, each once
- walk: int32 [32], P('tm'), may hold values from 0 to 63
- cfar_guard: int32 [2048], P('tm'), may hold values from 1 to 8
- cfar_window: int32 [2048], P('tm'), may hold values from 1 to 16
Outputs:
- detection: float32 [8192, 512], P(('chan', 'tm')), parts along dimension 0
The draws below stay inside these ranges and needn't reach their ends.
There are 4 independent parts, one for each index of `chan`. The reference program is written for one: setup_inputs(seed, part) draws one part's arguments, and reference() takes and returns one part's arrays. A program takes and returns all parts, laid end to end along the dimension named above; an argument that names none is the same for every part. Nothing has to cross between parts.
Inputs may be any that keep to these rules, and one draw needn't show every extreme that they name: block_ids names each of 0 to 31 exactly once.
All inputs are finite; a program needn't handle non-finite values.
Results may differ from the reference program's by a relative error of at most 0.0003.
Values sent between devices are 32-bit elements; how exact they have to be, the bound alone decides.
No kernel may reach another device: no remote copies, remote signals or barrier semaphores. Data moves between devices by JAX's collectives and lax.ppermute only.
A program may use at most 64 MiB of HBM per device.

```python
import math
import jax
import jax.numpy as jnp
from jax import lax

D = 2048
DOP = 512
SEGS = 64
GUARD_MAX = 8
WIN_MAX = 16
WALK = 64
NB = 32
L = 131072


def plant(values, own_key, smallest, high):
    place = [jax.random.randint(jax.random.fold_in(own_key, axis), (), 0, length) for axis, length in enumerate(values.shape)]
    main_axis = values.shape.index(max(values.shape))
    neighbour = place[:main_axis] + [(place[main_axis] + 1) % values.shape[main_axis]] + place[main_axis + 1:]
    return values.at[tuple(place)].set(smallest).at[tuple(neighbour)].set(high)


def levels(key, shape, cuts, low, largest):
    gain = 1.0
    for dim, shards_of in cuts:
        heights = jax.random.uniform(jax.random.fold_in(jax.random.fold_in(key, 6), dim), (shards_of,), jnp.float32, low / len(cuts), largest / len(cuts))
        gain = gain * jnp.repeat(jnp.exp(heights), shape[dim] // shards_of).reshape((-1,) + (1,) * (len(shape) - 1 - dim))
    return gain


def gaussian(key, shape, scale, bound, pieces=(), kind=jnp.bfloat16):
    result = jax.random.normal(key, shape, jnp.float32) * scale
    if len(pieces) > 0:
        result = levels(key, shape, pieces, -0.22, 0.18) * result
    return jnp.clip(result, min=-bound, max=bound).astype(kind)


def setup_inputs(seed: int = 0, part: int = 0) -> dict:
    keys = jax.random.split(jax.random.key(seed), 7)
    part_splits = jax.random.split(jax.random.fold_in(keys[6], part), 7)
    surveillance = gaussian(part_splits[0], (NB, L // 128, 256), 1.0, 6.0, ((0, 8),))
    ref_samples = gaussian(keys[1], (NB, (L + D) // 128, 256), 1.0, 6.0, ((0, 8),))
    block_ids = jax.random.permutation(keys[2], NB).astype(jnp.int32)
    walk = plant(jax.random.randint(keys[3], (NB,), 0, WALK), jax.random.fold_in(keys[3], 1), 0, WALK - 1).astype(jnp.int32)
    cfar_guard = plant(jax.random.randint(keys[4], (D,), 1, GUARD_MAX + 1), jax.random.fold_in(keys[4], 1), 1, GUARD_MAX).astype(jnp.int32)
    cfar_window = plant(jax.random.randint(keys[5], (D,), 1, WIN_MAX + 1), jax.random.fold_in(keys[5], 1), 1, WIN_MAX).astype(jnp.int32)
    return dict(surveillance=surveillance, ref_samples=ref_samples, block_ids=block_ids, walk=walk, cfar_guard=cfar_guard, cfar_window=cfar_window)


HIGH = lax.Precision.HIGHEST

def unpack(packed):
    count = packed.shape[0]
    real_part = packed[:, :, :128].astype(jnp.float32).reshape(count, -1)
    imag_part = packed[:, :, 128:].astype(jnp.float32).reshape(count, -1)
    return lax.complex(real_part, imag_part)

def correlate(item):
    surv_line, ref_line, shift = item
    segment = surv_line.reshape(SEGS, D)
    padded = jnp.concatenate([segment, jnp.zeros_like(segment)], axis=1)
    first = ref_line[:SEGS * D].reshape(SEGS, D)
    second = ref_line[D:].reshape(SEGS, D)
    window = jnp.concatenate([first, second], axis=1)
    spectrum = lax.optimization_barrier(jnp.sum(jnp.fft.fft(padded, axis=1) * jnp.conj(jnp.fft.fft(window, axis=1)), axis=0))
    lagged = jnp.fft.ifft(spectrum)
    picked = lax.dynamic_slice_in_dim(lagged, (D - shift).astype(jnp.int32), D)
    keep = jnp.arange(D, dtype=jnp.int32) >= shift
    return (jnp.where(keep, jnp.real(picked), 0.0), jnp.where(keep, jnp.imag(picked), 0.0))

def reference(surveillance, ref_samples, block_ids, walk, cfar_guard, cfar_window):
    real_c, imag_c = lax.map(correlate, (unpack(surveillance), unpack(ref_samples), walk))
    norm = 1.0 / math.sqrt(NB * SEGS * D)
    freq = jnp.arange(DOP, dtype=jnp.int32)
    theta = 2.0 * math.pi / DOP * (block_ids[:, None] * freq[None, :] % DOP).astype(jnp.float32)
    cos_table = jnp.cos(theta)
    sin_table = jnp.sin(theta)
    amp_re = (jnp.dot(real_c.T, cos_table, precision=HIGH) + jnp.dot(imag_c.T, sin_table, precision=HIGH)) * norm
    amp_im = (jnp.dot(imag_c.T, cos_table, precision=HIGH) - jnp.dot(real_c.T, sin_table, precision=HIGH)) * norm
    power = amp_re * amp_re + amp_im * amp_im
    floor = lax.optimization_barrier(jnp.sum(real_c * real_c + imag_c * imag_c, axis=0)) / (NB * SEGS * D)
    guard = cfar_guard
    width = cfar_window
    reach = GUARD_MAX + WIN_MAX
    padded = jnp.pad(power, ((reach, reach), (0, 0)))
    valid = jnp.pad(jnp.ones((D,), jnp.float32), (reach, reach))
    delay_sum = jnp.zeros_like(power)
    doppler_sum = jnp.zeros_like(power)
    count = jnp.zeros((D,), jnp.float32)
    for step in range(1, reach + 1):
        active = ((step > guard) & (step <= guard + width)).astype(jnp.float32)
        delay_sum = delay_sum + active[:, None] * (padded[reach + step:reach + step + D] + padded[reach - step:reach - step + D])
        count = count + active * (valid[reach + step:reach + step + D] + valid[reach - step:reach - step + D])
        doppler_sum = doppler_sum + active[:, None] * (jnp.roll(power, -step, axis=1) + jnp.roll(power, step, axis=1))
    noise = (delay_sum + doppler_sum) / (count[:, None] + 2.0 * width.astype(jnp.float32)[:, None])
    return (power - floor[:, None]) / (0.25 + noise)
```

```python
import functools
import math

import jax
import jax.numpy as jnp
from jax import lax
from jax.experimental import pallas as pl
from jax.experimental.pallas import tpu as pltpu
from jax.sharding import PartitionSpec as P

D = 2048
DOP = 512
SEGS = 64
GUARD_MAX = 8
WIN_MAX = 16
REACH = GUARD_MAX + WIN_MAX
LANES = 128
LAGS = D // LANES
GROUP = 64

HIGH = lax.Precision.HIGHEST


def correlate_kernel(walk, ids, surv, ref, out, surv_f, ref_f, keys, waves, grams, skewed, natural, *, span):
    step = pl.program_id(0)
    blocks = pl.num_programs(0)
    rows = surv.shape[1]
    members = rows // GROUP
    for half in range(2):
        lanes = slice(half * LANES, (half + 1) * LANES)
        surv_f[half] = surv[0, :, lanes].astype(jnp.float32)
        ref_f[half] = ref[0, :, lanes].astype(jnp.float32)
    for half in range(2):
        lanes = slice(half * LANES, (half + 1) * LANES)
        for sigma in range(0, GROUP, LANES // members):
            tile = jnp.concatenate(
                [surv_f[half, pl.ds(sigma + i, members, stride=GROUP), :] for i in range(LANES // members)], 0
            )
            keys[lanes, sigma * members : sigma * members + LANES] = tile.T.astype(jnp.bfloat16)
        for sigma in range(GROUP + LAGS):
            waves[sigma * members : (sigma + 1) * members, lanes] = ref_f[
                half, pl.ds(sigma, members, stride=GROUP), :
            ].astype(jnp.bfloat16)
    for b in range(LAGS + 1):
        gram = jnp.dot(
            keys[...], waves[b * members : b * members + rows, :], preferred_element_type=jnp.float32
        )
        grams[b, 0] = gram[:LANES, :LANES] + gram[LANES:, LANES:]
        grams[b, 1] = gram[LANES:, :LANES] - gram[:LANES, LANES:]
    sub = lax.broadcasted_iota(jnp.int32, (8, LANES), 0)
    lane = lax.broadcasted_iota(jnp.int32, (8, LANES), 1)
    for b in range(LAGS):
        for part in range(2):
            total = None
            for i in range(LANES // 8):
                own = slice(8 * i, 8 * i + 8)
                mixed = jnp.where(lane > 8 * i + sub, grams[b, part, own], grams[b + 1, part, own])
                if i:
                    mixed = pltpu.roll(mixed, LANES - 8 * i, 1)
                total = mixed if total is None else total + mixed
            at = 8 * (part * LAGS + LAGS - 1 - b)
            skewed[at : at + 8] = total
    summed = None
    for s in range(8):
        line = pltpu.roll(skewed[pl.ds(s, 2 * LAGS, stride=8), :], LANES - s - 1, 1)
        summed = line if summed is None else summed + line
    natural[pl.ds(pl.multiple_of(step * 2 * LAGS, 2 * LAGS), 2 * LAGS), :] = summed

    @pl.when(step == blocks - 1)
    def finish():
        count = natural.shape[0] // (2 * LAGS)
        here = lax.broadcasted_iota(jnp.int32, (LANES, LANES), 0)
        there = lax.broadcasted_iota(jnp.int32, (LANES, LANES), 1)
        flip = (here + there == LANES - 1).astype(jnp.float32)
        delays = jnp.dot(natural[...], flip, precision=HIGH, preferred_element_type=jnp.float32)
        spot = lax.broadcasted_iota(jnp.int32, (LAGS, LANES), 1)
        for row in range(2 * count):
            shift = walk[row // 2]
            moved = pltpu.roll(delays[row * LAGS : (row + 1) * LAGS], shift, 1)
            below = jnp.concatenate([jnp.zeros((1, LANES), jnp.float32), moved[:-1]], 0)
            natural[row * LAGS : (row + 1) * LAGS, :] = jnp.where(spot >= shift, moved, below)
        if span % LANES:
            out[...] = natural[...]
            return
        tiles = span // LANES
        name = jnp.concatenate(
            [jnp.full((1, LANES), ids[row // 2].astype(jnp.float32), jnp.float32) for row in range(2 * count)], 0
        )
        at = lax.broadcasted_iota(jnp.int32, (2 * count, LANES), 1)
        nothing = jnp.zeros((2 * count, LANES), jnp.float32)

        def lag_row(k):
            if k < 0 or k >= LAGS:
                return nothing
            return natural[pl.ds(k, 2 * count, stride=LAGS), :]

        for dest in range(LAGS // tiles):
            for k in range(tiles):
                out[dest, :, k * LANES : (k + 1) * LANES] = lag_row(dest * tiles + k)
            halo = jnp.where(at < 32, lag_row((dest + 1) * tiles), lag_row(dest * tiles - 1))
            out[dest, :, tiles * LANES :] = jnp.where((at >= 32) & (at < 96), name, halo)


def correlate(surveillance, ref_samples, walk, ids, devices):
    blocks, rows, _ = surveillance.shape
    ref_rows = ref_samples.shape[1]
    span = D // devices
    width = window_width(span)
    direct = span % LANES == 0
    shape = (devices, 2 * blocks, width) if direct else (2 * blocks * LAGS, LANES)
    result = pl.pallas_call(
        functools.partial(correlate_kernel, span=span),
        out_shape=jax.ShapeDtypeStruct(shape, jnp.float32),
        grid_spec=pltpu.PrefetchScalarGridSpec(
            num_scalar_prefetch=2,
            grid=(blocks,),
            in_specs=[
                pl.BlockSpec((1, rows, 256), lambda i, *_: (i, 0, 0)),
                pl.BlockSpec((1, ref_rows, 256), lambda i, *_: (i, 0, 0)),
            ],
            out_specs=pl.BlockSpec(shape, lambda i, *_: (0,) * len(shape)),
            scratch_shapes=[
                pltpu.VMEM((2, rows, LANES), jnp.float32),
                pltpu.VMEM((2, ref_rows, LANES), jnp.float32),
                pltpu.VMEM((256, rows), jnp.bfloat16),
                pltpu.VMEM((rows + LAGS * (rows // GROUP), 256), jnp.bfloat16),
                pltpu.VMEM((LAGS + 1, 2, LANES, LANES), jnp.float32),
                pltpu.VMEM((2 * LAGS * 8, LANES), jnp.float32),
                pltpu.VMEM((2 * blocks * LAGS, LANES), jnp.float32),
            ],
        ),
        compiler_params=pltpu.CompilerParams(dimension_semantics=("arbitrary",)),
    )(walk, ids, surveillance, ref_samples)
    if direct:
        return result
    flat = result.reshape(2 * blocks, D)
    names = jnp.repeat(ids.astype(jnp.float32), 2)[:, None]
    padded = jnp.pad(flat, ((0, 0), (REACH, REACH)))
    fill = jnp.broadcast_to(names, (2 * blocks, width - span - 2 * REACH))
    return jnp.stack(
        [
            jnp.concatenate(
                [
                    padded[:, p * span + REACH : (p + 1) * span + 2 * REACH],
                    fill,
                    padded[:, p * span : p * span + REACH],
                ],
                1,
            )
            for p in range(devices)
        ]
    )


def window_width(span):
    return -(-(span + 2 * REACH + 16) // LANES) * LANES


def split(x):
    top = x.astype(jnp.bfloat16)
    return top, (x - top.astype(jnp.float32)).astype(jnp.bfloat16)


def cosine(turn):
    turn = turn & (DOP - 1)
    turn = jnp.minimum(turn, DOP - turn)
    x = (DOP // 4 - turn).astype(jnp.float32) * (2.0 * math.pi / DOP)
    y = x * x
    poly = 1.0
    for n in (13, 11, 9, 7, 5, 3):
        poly = 1.0 - y * poly * (1.0 / (n * (n - 1)))
    return x * poly


def detect_kernel(base, moved, cells, out, power, delay, sizes, *, norm):
    span = out.shape[0]
    sources, lines, width = moved.shape
    stacked = moved[...].reshape(sources * lines, width)
    count = sources * lines
    ids = stacked[:, span + 32 : span + 33].astype(jnp.int32)
    freq = lax.broadcasted_iota(jnp.int32, (count, DOP), 1)
    imag = lax.broadcasted_iota(jnp.int32, (count, DOP), 0) & 1
    turn = ids * freq - imag * (DOP // 4)
    mixer = jnp.concatenate([cosine(turn), cosine(turn + DOP // 4)], 1)
    top, rest = split(stacked * norm)
    mix_top, mix_rest = split(mixer)
    amp = lax.dot_general(
        jnp.concatenate([top, top, rest], 0),
        jnp.concatenate([mix_top, mix_rest, mix_top], 0),
        (((0,), (0,)), ((), ())),
        preferred_element_type=jnp.float32,
    )
    whole = amp[:, :DOP] * amp[:, :DOP] + amp[:, DOP:] * amp[:, DOP:]
    power[...] = whole[:span]
    tile = cells.shape[1]
    for k in range(cells.shape[0]):
        spread = jnp.broadcast_to(cells[k : k + 1, :].astype(jnp.float32), (tile, tile)).T
        sizes[k * tile : (k + 1) * tile, :] = spread[:, :1].astype(jnp.int32)
    packed = sizes[...]
    guard = packed & 31
    reach = guard + (packed >> 5)
    place = lax.broadcasted_iota(jnp.int32, (span, width), 1)
    place = jnp.where(place < span + 32, place, place - width)
    dist = jnp.abs(place - lax.broadcasted_iota(jnp.int32, (span, width), 0))
    spot = place + base[0]
    band = (dist > guard) & (dist <= reach) & (spot >= 0) & (spot < D)
    band = jnp.where(band, 1.0, 0.0)
    tally = jnp.sum(band, axis=1, keepdims=True)
    band = band.astype(jnp.bfloat16)
    top, rest = split(whole)
    delay[...] = (
        jnp.dot(band, top, preferred_element_type=jnp.float32)
        + jnp.dot(band, rest, preferred_element_type=jnp.float32)
    )
    weight = 1.0 / (tally + 2.0 * (reach - guard).astype(jnp.float32))
    rows = 16
    for k in range(span // rows):
        own = slice(k * rows, (k + 1) * rows)
        cell = power[own]
        low = guard[own]
        high = reach[own]
        wide = high - low

        def ahead(x, n):
            return pltpu.roll(x, DOP - n, 1)

        sums = [cell]
        for e in range(4):
            sums.append(sums[-1] + ahead(sums[-1], 1 << e))
        near = jnp.where((wide & 16) > 0, sums[4], 0.0)
        for e in (3, 2, 1, 0):
            near = jnp.where((wide & (1 << e)) > 0, sums[e] + ahead(near, 1 << e), near)
        right = near
        for e in range(4):
            right = jnp.where(((low + 1) & (1 << e)) > 0, ahead(right, 1 << e), right)
        left = near
        for e in range(5):
            left = jnp.where((high & (1 << e)) > 0, pltpu.roll(left, 1 << e, 1), left)
        level = jnp.sum(cell, axis=1, keepdims=True) * (1.0 / DOP)
        noise = (delay[own] + left + right) * weight[own]
        out[own] = (cell - level) / (0.25 + noise)


def detect(moved, base, guard, window, norm):
    span = guard.shape[0]
    width = moved.shape[2]
    tile = min(span, LANES)
    cells = (guard + 32 * window).reshape(span // tile, tile)
    whole = pl.BlockSpec(memory_space=pltpu.VMEM)
    return pl.pallas_call(
        functools.partial(detect_kernel, norm=norm),
        out_shape=jax.ShapeDtypeStruct((span, DOP), jnp.float32),
        in_specs=[pl.BlockSpec(memory_space=pltpu.SMEM), whole, whole],
        out_specs=whole,
        scratch_shapes=[
            pltpu.VMEM((span, DOP), jnp.float32),
            pltpu.VMEM((span, DOP), jnp.float32),
            pltpu.VMEM((span, 1), jnp.int32),
        ],
    )(base, moved, cells)


def body(surveillance, ref_samples, block_ids, walk, cfar_guard, cfar_window):
    blocks = surveillance.shape[0]
    devices = lax.axis_size("tm")
    norm = 1.0 / math.sqrt(blocks * devices * SEGS * D)
    windows = correlate(surveillance, ref_samples, walk, block_ids, devices)
    moved = lax.all_to_all(windows, "tm", split_axis=0, concat_axis=0, tiled=True)
    base = (lax.axis_index("tm") * (D // devices)).astype(jnp.int32).reshape(1)
    return detect(moved, base, cfar_guard, cfar_window, norm)


def solution(mesh):
    in_specs = (
        P(("chan", "tm"), None, None),
        P("tm", None, None),
        P("tm"),
        P("tm"),
        P("tm"),
        P("tm"),
    )
    out_specs = P(("chan", "tm"), None)
    return jax.shard_map(body, mesh=mesh, in_specs=in_specs, out_specs=out_specs, check_vma=False)
```

```python
import functools
import math

import jax
import jax.numpy as jnp
from jax import lax
from jax.experimental import pallas as pl
from jax.experimental.pallas import tpu as pltpu
from jax.sharding import PartitionSpec as P

D = 2048
DOP = 512
SEGS = 64
GUARD_MAX = 8
WIN_MAX = 16
REACH = GUARD_MAX + WIN_MAX
LANES = 128
LAGS = D // LANES
GROUP = 8

HIGH = lax.Precision.HIGHEST


def correlate_kernel(walk, ids, surv, ref, out, surv_f, ref_f, keys, waves, grams, skewed, natural, *, span):
    step = pl.program_id(0)
    blocks = pl.num_programs(0)
    rows = surv.shape[1]
    members = rows // GROUP
    for half in range(2):
        lanes = slice(half * LANES, (half + 1) * LANES)
        surv_f[half] = surv[0, :, lanes].astype(jnp.float32)
        ref_f[half] = ref[0, :, lanes].astype(jnp.float32)
    for half in range(2):
        lanes = slice(half * LANES, (half + 1) * LANES)
        for sigma in range(0, GROUP, LANES // members):
            tile = jnp.concatenate(
                [surv_f[half, pl.ds(sigma + i, members, stride=GROUP), :] for i in range(LANES // members)], 0
            )
            keys[lanes, sigma * members : sigma * members + LANES] = tile.T.astype(jnp.bfloat16)
        for sigma in range(GROUP + LAGS):
            waves[sigma * members : (sigma + 1) * members, lanes] = ref_f[
                half, pl.ds(sigma, members, stride=GROUP), :
            ].astype(jnp.bfloat16)
    for b in range(LAGS + 1):
        gram = jnp.dot(
            keys[...], waves[b * members : b * members + rows, :], preferred_element_type=jnp.float32
        )
        grams[b, 0] = gram[:LANES, :LANES] + gram[LANES:, LANES:]
        grams[b, 1] = gram[LANES:, :LANES] - gram[:LANES, LANES:]
    sub = lax.broadcasted_iota(jnp.int32, (8, LANES), 0)
    lane = lax.broadcasted_iota(jnp.int32, (8, LANES), 1)
    for b in range(LAGS):
        for part in range(2):
            total = None
            for i in range(LANES // 8):
                own = slice(8 * i, 8 * i + 8)
                mixed = jnp.where(lane > 8 * i + sub, grams[b, part, own], grams[b + 1, part, own])
                if i:
                    mixed = pltpu.roll(mixed, LANES - 8 * i, 1)
                total = mixed if total is None else total + mixed
            at = 8 * (part * LAGS + LAGS - 1 - b)
            skewed[at : at + 8] = total
    summed = None
    for s in range(8):
        line = pltpu.roll(skewed[pl.ds(s, 2 * LAGS, stride=8), :], LANES - s - 1, 1)
        summed = line if summed is None else summed + line
    natural[pl.ds(pl.multiple_of(step * 2 * LAGS, 2 * LAGS), 2 * LAGS), :] = summed

    @pl.when(step == blocks - 1)
    def finish():
        count = natural.shape[0] // (2 * LAGS)
        here = lax.broadcasted_iota(jnp.int32, (LANES, LANES), 0)
        there = lax.broadcasted_iota(jnp.int32, (LANES, LANES), 1)
        flip = (here + there == LANES - 1).astype(jnp.float32)
        delays = jnp.dot(natural[...], flip, precision=HIGH, preferred_element_type=jnp.float32)
        spot = lax.broadcasted_iota(jnp.int32, (LAGS, LANES), 1)
        for row in range(2 * count):
            shift = walk[row // 2]
            moved = pltpu.roll(delays[row * LAGS : (row + 1) * LAGS], shift, 1)
            below = jnp.concatenate([jnp.zeros((1, LANES), jnp.float32), moved[:-1]], 0)
            natural[row * LAGS : (row + 1) * LAGS, :] = jnp.where(spot >= shift, moved, below)
        if span % LANES:
            out[...] = natural[...]
            return
        tiles = span // LANES
        name = jnp.concatenate(
            [jnp.full((1, LANES), ids[row // 2].astype(jnp.float32), jnp.float32) for row in range(2 * count)], 0
        )
        at = lax.broadcasted_iota(jnp.int32, (2 * count, LANES), 1)
        nothing = jnp.zeros((2 * count, LANES), jnp.float32)

        def lag_row(k):
            if k < 0 or k >= LAGS:
                return nothing
            return natural[pl.ds(k, 2 * count, stride=LAGS), :]

        for dest in range(LAGS // tiles):
            for k in range(tiles):
                out[dest, :, k * LANES : (k + 1) * LANES] = lag_row(dest * tiles + k)
            halo = jnp.where(at < 32, lag_row((dest + 1) * tiles), lag_row(dest * tiles - 1))
            out[dest, :, tiles * LANES :] = jnp.where((at >= 32) & (at < 96), name, halo)


def correlate(surveillance, ref_samples, walk, ids, devices):
    blocks, rows, _ = surveillance.shape
    ref_rows = ref_samples.shape[1]
    span = D // devices
    width = window_width(span)
    direct = span % LANES == 0
    shape = (devices, 2 * blocks, width) if direct else (2 * blocks * LAGS, LANES)
    result = pl.pallas_call(
        functools.partial(correlate_kernel, span=span),
        out_shape=jax.ShapeDtypeStruct(shape, jnp.float32),
        grid_spec=pltpu.PrefetchScalarGridSpec(
            num_scalar_prefetch=2,
            grid=(blocks,),
            in_specs=[
                pl.BlockSpec((1, rows, 256), lambda i, *_: (i, 0, 0)),
                pl.BlockSpec((1, ref_rows, 256), lambda i, *_: (i, 0, 0)),
            ],
            out_specs=pl.BlockSpec(shape, lambda i, *_: (0,) * len(shape)),
            scratch_shapes=[
                pltpu.VMEM((2, rows, LANES), jnp.float32),
                pltpu.VMEM((2, ref_rows, LANES), jnp.float32),
                pltpu.VMEM((256, rows), jnp.bfloat16),
                pltpu.VMEM((rows + LAGS * (rows // GROUP), 256), jnp.bfloat16),
                pltpu.VMEM((LAGS + 1, 2, LANES, LANES), jnp.float32),
                pltpu.VMEM((2 * LAGS * 8, LANES), jnp.float32),
                pltpu.VMEM((2 * blocks * LAGS, LANES), jnp.float32),
            ],
        ),
        compiler_params=pltpu.CompilerParams(dimension_semantics=("arbitrary",)),
    )(walk, ids, surveillance, ref_samples)
    if direct:
        return result
    flat = result.reshape(2 * blocks, D)
    names = jnp.repeat(ids.astype(jnp.float32), 2)[:, None]
    padded = jnp.pad(flat, ((0, 0), (REACH, REACH)))
    fill = jnp.broadcast_to(names, (2 * blocks, width - span - 2 * REACH))
    return jnp.stack(
        [
            jnp.concatenate(
                [
                    padded[:, p * span + REACH : (p + 1) * span + 2 * REACH],
                    fill,
                    padded[:, p * span : p * span + REACH],
                ],
                1,
            )
            for p in range(devices)
        ]
    )


def window_width(span):
    return -(-(span + 2 * REACH + 16) // LANES) * LANES


def split(x):
    top = x.astype(jnp.bfloat16)
    return top, (x - top.astype(jnp.float32)).astype(jnp.bfloat16)


def cosine(turn):
    turn = turn & (DOP - 1)
    turn = jnp.minimum(turn, DOP - turn)
    x = (DOP // 4 - turn).astype(jnp.float32) * (2.0 * math.pi / DOP)
    y = x * x
    poly = 1.0
    for n in (13, 11, 9, 7, 5, 3):
        poly = 1.0 - y * poly * (1.0 / (n * (n - 1)))
    return x * poly


def detect_kernel(base, moved, cells, out, *, norm):
    span = out.shape[0]
    sources, lines, width = moved.shape
    count = sources * lines
    stacked = moved[...].reshape(count, width)
    names = stacked[:, width - LANES :]
    names = jnp.concatenate([names, names], 0).T
    at = span + 32 - (width - LANES)
    ids = names[at : at + 1, :].astype(jnp.int32)
    freq = lax.broadcasted_iota(jnp.int32, (DOP, 2 * count), 0)
    imag = lax.broadcasted_iota(jnp.int32, (DOP, 2 * count), 1) & 1
    mix_top, mix_rest = split(cosine(ids * freq - imag * (DOP // 4)))
    stacked = stacked * norm
    even = lax.broadcasted_iota(jnp.int32, (count, width), 0) & 1 == 0
    turned = jnp.where(even, pltpu.roll(stacked, count - 1, 0), -pltpu.roll(stacked, 1, 0))
    top, rest = split(jnp.concatenate([stacked, turned], 1))
    amp = jnp.dot(
        jnp.concatenate([mix_top, mix_rest], 1),
        jnp.concatenate([top, rest, top, rest], 0),
        preferred_element_type=jnp.float32,
    )
    whole = amp[:, :width] * amp[:, :width] + amp[:, width:] * amp[:, width:]
    top, rest = split(whole)
    tile = cells.shape[1]
    for k in range(cells.shape[0]):
        packed = cells[k : k + 1, :]
        low = packed & 31
        wide = packed >> 5
        high = low + wide
        place = lax.broadcasted_iota(jnp.int32, (width, tile), 0)
        place = jnp.where(place < span + 32, place, place - width)
        dist = jnp.abs(place - k * tile - lax.broadcasted_iota(jnp.int32, (width, tile), 1))
        spot = place + base[0]
        band = (dist > low) & (dist <= high) & (spot >= 0) & (spot < D)
        band = jnp.where(band, 1.0, 0.0)
        tally = jnp.sum(band, axis=0, keepdims=True)
        band = band.astype(jnp.bfloat16)
        delay = jnp.dot(top, band, preferred_element_type=jnp.float32) + jnp.dot(
            rest, band, preferred_element_type=jnp.float32
        )
        weight = 1.0 / (tally + 2.0 * wide.astype(jnp.float32))
        cell = whole[:, k * tile : (k + 1) * tile]

        def ahead(x, n):
            return pltpu.roll(x, DOP - n, 0)

        def has(x, e):
            return (x & (1 << e)) > 0

        sums = [cell]
        for e in range(4):
            sums.append(sums[-1] + ahead(sums[-1], 1 << e))
        near = jnp.where(has(wide, 4), sums[4], 0.0)
        for e in (3, 2, 1, 0):
            near = jnp.where(has(wide, e), sums[e] + ahead(near, 1 << e), near)
        right = near
        for e in range(4):
            right = jnp.where(has(low + 1, e), ahead(right, 1 << e), right)
        left = near
        for e in range(5):
            left = jnp.where(has(high, e), pltpu.roll(left, 1 << e, 0), left)
        level = jnp.sum(cell, axis=0, keepdims=True) * (1.0 / DOP)
        noise = (delay + left + right) * weight
        out[k * tile : (k + 1) * tile, :] = ((cell - level) / (0.25 + noise)).T


def detect(moved, base, guard, window, norm):
    span = guard.shape[0]
    width = moved.shape[2]
    tile = min(span, LANES)
    cells = (guard + 32 * window).reshape(span // tile, tile)
    whole = pl.BlockSpec(memory_space=pltpu.VMEM)
    return pl.pallas_call(
        functools.partial(detect_kernel, norm=norm),
        out_shape=jax.ShapeDtypeStruct((span, DOP), jnp.float32),
        in_specs=[pl.BlockSpec(memory_space=pltpu.SMEM), whole, whole],
        out_specs=whole,
    )(base, moved, cells)


def body(surveillance, ref_samples, block_ids, walk, cfar_guard, cfar_window):
    blocks = surveillance.shape[0]
    devices = lax.axis_size("tm")
    norm = 1.0 / math.sqrt(blocks * devices * SEGS * D)
    windows = correlate(surveillance, ref_samples, walk, block_ids, devices)
    moved = lax.all_to_all(windows, "tm", split_axis=0, concat_axis=0, tiled=True)
    base = (lax.axis_index("tm") * (D // devices)).astype(jnp.int32).reshape(1)
    return detect(moved, base, cfar_guard, cfar_window, norm)


def solution(mesh):
    in_specs = (
        P(("chan", "tm"), None, None),
        P("tm", None, None),
        P("tm"),
        P("tm"),
        P("tm"),
        P("tm"),
    )
    out_specs = P(("chan", "tm"), None)
    return jax.shard_map(body, mesh=mesh, in_specs=in_specs, out_specs=out_specs, check_vma=False)
```
